32 devices in a mesh: group: 4 (over y, x), rank: 8 (over z, core).
Axes of the slice: x: 2, y: 2, z: 4, core: 2. Of those that a mesh axis runs over, the one named last changes fastest.
Arguments:
- queries: bfloat16 [8192, 2048], P(('group', 'rank')), may hold values from -32 to 32
- key_rows: bfloat16 [8192, 2048], P(('group', 'rank')), may hold values from -6 to 6
- value_rows: bfloat16 [8192, 2048], P(('group', 'rank')), may hold values from -6 to 6
- tile_links: int32 [64, 8], P(('group', 'rank')), may hold values from 0 to 15, as said below
- link_counts: int32 [64], P(('group', 'rank')), may hold values from 1 to 8, 256 in all
Outputs:
- attended: bfloat16 [8192, 2048], P(('group', 'rank'))
The draws below stay inside these ranges and needn't reach their ends.
Inputs may be any that keep to these rules, and one draw needn't show every extreme that they name: `tile_links`: each row names 8 different candidates.
All inputs are finite; a program needn't handle non-finite values. No bound on the sum of `link_counts` on one device may be relied on, other than what follows from the above.
Results may differ from the reference program's by a relative error of at most 0.0045.
Values may be sent and summed in bfloat16 or wider, within the bound.
A program may use at most 128 MiB of HBM per device.

```python
import math
import jax
import jax.numpy as jnp
import numpy as np
from jax import lax

H = 16
HD = 128
TILE = 128
TPD = 2
LMAX = 8
W = 2048
GROUPS = 4
RANKS = 8
NTILES = 64
NODES = 8192
CAND = 16


def shared_rows(key):
    base = jax.random.fold_in(key, 7)
    query_key, key_key = jax.random.split(base, 2)
    query_draw = jnp.clip(jax.random.normal(query_key, (NODES, W), jnp.float32), -6.0, 6.0)
    key_draw = jnp.clip(jax.random.normal(key_key, (NODES, W), jnp.float32), -6.0, 6.0)
    return (query_draw, key_draw)


def draw_queries(key, part):
    return shared_rows(key)[0].astype(jnp.bfloat16)


def draw_key_rows(key, part):
    return shared_rows(key)[1].astype(jnp.bfloat16)


def draw_tile_links(key, part):
    link_key = jax.random.fold_in(key, 11)
    scores = jax.random.randint(link_key, (NTILES, CAND), 0, 2 ** 20) * CAND + jnp.arange(CAND, dtype=jnp.int32)[None, :]
    order = jnp.argsort(scores, axis=1)
    return order[:, :LMAX].astype(jnp.int32)


def level_of(key, dims, cuts, smallest, high):
    factor_of, own = 1.0, jax.random.fold_in(key, 6)
    for dim, blocks in cuts:
        heights = jnp.exp(jax.random.uniform(jax.random.fold_in(own, dim), (blocks,), jnp.float32, smallest / len(cuts), high / len(cuts)))
        factor_of = factor_of * jnp.repeat(heights, dims[dim] // blocks).reshape([-1 if axis == dim else 1 for axis in range(len(dims))])
    return factor_of


def length_profile(amount, total, bound, lean):
    portions = [(1 << 20) // math.isqrt(standing ** lean) + 1 for standing in range(2, amount + 1)]
    spare, counts = total - bound - (amount - 1), [1] * (amount - 1)
    while spare > 0:
        candidates = [i for i in range(amount - 1) if counts[i] < bound]
        whole, left = sum([portions[i] for i in candidates]), spare
        for i in candidates:
            more = min(bound - counts[i], max(1, left * portions[i] // whole), spare)
            counts[i] = counts[i] + more
            spare = spare - more
    return np.array([bound] + counts)


def ragged(key, amount, total, limit, lean):
    if amount == 2:
        one = jax.random.randint(key, (), max(1, total - limit), min(limit, total - 1) + 1)
        return jnp.stack([one, total - one])
    lengths = jnp.asarray(length_profile(amount, total, limit, lean), jnp.int32)
    pairs = (amount - 1) // 2
    giver, sink = lengths[1:1 + 2 * pairs:2], lengths[2:2 + 2 * pairs:2]
    room = jnp.minimum(giver - 1, limit - sink)
    passed = jax.random.randint(jax.random.fold_in(key, 1), (pairs,), 0, 1 << 20) % (room + 1)
    lengths = lengths.at[1:1 + 2 * pairs:2].set(giver - passed).at[2:2 + 2 * pairs:2].set(sink + passed)
    return lengths[jax.random.permutation(jax.random.fold_in(key, 2), amount)]


def centred(key, dims, scale, limit, cuts=(), kind=jnp.bfloat16):
    values = jax.random.normal(key, dims, jnp.float32) * scale
    if len(cuts) > 0:
        values = level_of(key, dims, cuts, -0.22, 0.18) * values
    return jnp.clip(values, min=-limit, max=limit).astype(kind)


def setup_inputs(seed: int = 0) -> dict:
    splits = jax.random.split(jax.random.key(seed), 6)
    queries = draw_queries(jax.random.fold_in(splits[5], 71), 0)
    key_rows = draw_key_rows(jax.random.fold_in(splits[5], 71), 0)
    value_rows = centred(splits[2], (NODES, W), 1.0, 6.0, ((0, 32),))
    tile_links = draw_tile_links(jax.random.fold_in(splits[5], 71), 0)
    link_counts = ragged(splits[4], NTILES, NTILES * LMAX // 2, LMAX, 2).astype(jnp.int32)
    return dict(queries=queries, key_rows=key_rows, value_rows=value_rows, tile_links=tile_links, link_counts=link_counts)


def candidate_tiles(tile_id, slot_ids):
    device = tile_id // TPD
    group_id = device // RANKS
    range_id = device % RANKS
    within = slot_ids % TPD
    block_id = slot_ids // TPD
    offsets = jnp.array([-2, -1, 1, 2], jnp.int32)
    beside = offsets[jnp.clip(block_id - 1, 0, 3)]
    beside_range = (range_id + beside) % RANKS
    peer_group = (group_id + block_id - 4) % GROUPS
    local_tile = device * TPD + within
    beside_tile = (group_id * RANKS + beside_range) * TPD + within
    peer_tile = (peer_group * RANKS + range_id) * TPD + within
    chosen = jnp.where(block_id == 0, local_tile, jnp.where(block_id <= 4, beside_tile, peer_tile))
    return chosen.astype(jnp.int32)


def softmax_mix(query_tile, chosen_keys, chosen_values, usable):
    scores = jnp.einsum("qhd,khd->hqk", query_tile, chosen_keys) * (HD ** -0.5)
    key_mask = jnp.repeat(usable, TILE)
    scores = jnp.where(key_mask[None, None, :], scores, -jnp.inf)
    row_max = jnp.max(scores, axis=-1, keepdims=True)
    weights = jnp.exp(scores - row_max)
    row_total = jnp.sum(weights, axis=-1)
    rounded = weights.astype(jnp.bfloat16)
    mixed_rows = jnp.einsum("hqk,khd->qhd", rounded.astype(jnp.float32), chosen_values)
    return (mixed_rows / jnp.transpose(row_total)[:, :, None]).reshape(TILE, W).astype(jnp.bfloat16)


def reference(queries, key_rows, value_rows, tile_links, link_counts):
    key_tiles = key_rows.reshape(NTILES, TILE, W)
    value_tiles = value_rows.reshape(NTILES, TILE, W)

    def one_tile(tile_id):
        first = jnp.reshape(tile_id % TPD, (1,)).astype(jnp.int32)
        slot_ids = jnp.concatenate([first, tile_links[tile_id].astype(jnp.int32)])
        global_ids = candidate_tiles(tile_id, slot_ids)
        chosen_keys = key_tiles[global_ids].reshape((LMAX + 1) * TILE, H, HD).astype(jnp.float32)
        chosen_values = value_tiles[global_ids].reshape((LMAX + 1) * TILE, H, HD).astype(jnp.float32)
        query_tile = lax.dynamic_slice_in_dim(queries, (tile_id * TILE).astype(jnp.int32), TILE, 0)
        query_tile = query_tile.reshape(TILE, H, HD).astype(jnp.float32)
        usable = jnp.concatenate([jnp.ones((1,), bool), jnp.arange(LMAX, dtype=jnp.int32) < link_counts[tile_id]])
        return softmax_mix(query_tile, chosen_keys, chosen_values, usable)

    result = lax.map(one_tile, jnp.arange(NTILES, dtype=jnp.int32))
    return result.reshape(NODES, W)
```

```python
import functools
import math

import jax
import jax.numpy as jnp
from jax import lax
from jax.experimental import pallas as pl
from jax.experimental.pallas import tpu as pltpu
from jax.sharding import PartitionSpec as P

HD = 128
CHUNK_SIXTEENTHS = (4, 4, 4, 2, 1, 1)
MESH = pl.DeviceIdType.MESH


def kernel(
    groups,
    ranks,
    bounds,
    q_hbm,
    k_hbm,
    v_hbm,
    links_hbm,
    counts_hbm,
    o_ref,
    land,
    q_v,
    bias,
    send_sems,
    recv_sems,
    q_sem,
    links,
    counts,
    list_sems,
    ready,
):
    _, slots, rows, _ = land.shape
    chunks = len(bounds) - 1
    tiles, lmax = links.shape
    tile_rows = rows // tiles
    g = lax.axis_index("group")
    r = lax.axis_index("rank")
    core = lax.rem(r, 2)
    partner = (g, r + 1 - 2 * core)
    crossed = groups == 4
    across = (g + 1 - 2 * lax.rem(g, 2), lax.rem(g + 2, 4))

    def peer_slot(source, at):
        return 4 + lax.rem(source - at + groups, groups)

    flows = [
        ((g, lax.rem(r + 2, ranks)), 1, 1),
        ((g, lax.rem(r + ranks - 2, ranks)), 4, 0),
    ]
    if crossed:
        for near in across:
            flows.append(((near, r), peer_slot(g, near), len(flows)))
    else:
        for step in range(1, groups):
            back = 1 + groups - step
            flows.append(((lax.rem(g + groups - step, groups), r), 4 + step, back))
    beside = len(flows)
    relay = beside + 1
    hops = (across, across[::-1])

    here = g * ranks + r
    before = [target[0] * ranks + target[1] < here for target, _, _ in flows]
    barrier = pltpu.get_barrier_semaphore()
    pl.semaphore_signal(barrier, inc=1, device_id=partner, device_id_type=MESH)
    greeted = 1
    for (device, _, _), earlier in zip(flows, before):
        greeted = greeted + jnp.where(earlier, 1, 0)

        @pl.when(jnp.logical_not(earlier))
        def _():
            pl.semaphore_signal(barrier, inc=1, device_id=device, device_id_type=MESH)

    def columns(c):
        return pl.ds(bounds[c] * HD, (bounds[c + 1] - bounds[c]) * HD)

    def own_copy(c, kv):
        src = (k_hbm, v_hbm)[kv]
        return pltpu.make_async_copy(
            src.at[:, columns(c)], land.at[kv, 0, :, columns(c)], recv_sems.at[c, kv, 0]
        )

    def flow_copy(c, kv, f):
        device, slot = (partner, 2 + core) if f == beside else flows[f][:2]
        src = (k_hbm, v_hbm)[kv]
        part = columns(c)
        return pltpu.make_async_remote_copy(
            src_ref=src.at[:, part],
            dst_ref=land.at[kv, slot, :, part],
            send_sem=send_sems.at[kv, f],
            recv_sem=recv_sems.at[c, kv, slot],
            device_id=device,
            device_id_type=MESH,
        )

    def relay_copy(c, kv):
        return pltpu.make_async_remote_copy(
            src_ref=land.at[kv, 4 - 3 * core, :, columns(c)],
            dst_ref=land.at[kv, 3 - core, :, columns(c)],
            send_sem=send_sems.at[kv, relay],
            recv_sem=recv_sems.at[c, kv, 3 - core],
            device_id=partner,
            device_id_type=MESH,
        )

    def cross_copy(c, kv):
        source, target = hops[kv]
        slot = peer_slot(source, target)
        return pltpu.make_async_remote_copy(
            src_ref=land.at[kv, peer_slot(source, g), :, columns(c)],
            dst_ref=land.at[kv, slot, :, columns(c)],
            send_sem=send_sems.at[kv, relay + 1],
            recv_sem=recv_sems.at[c, kv, slot],
            device_id=(target, r),
            device_id_type=MESH,
        )

    def arrived(c, kv, slot):
        pltpu.make_async_remote_copy(
            src_ref=land.at[kv, slot, :, columns(c)],
            dst_ref=land.at[kv, slot, :, columns(c)],
            send_sem=send_sems.at[kv, 0],
            recv_sem=recv_sems.at[c, kv, slot],
            device_id=partner,
            device_id_type=MESH,
        ).wait_recv()

    def sent(kv, f):
        whole = land.at[kv, 0]
        pltpu.make_async_remote_copy(
            src_ref=whole,
            dst_ref=whole,
            send_sem=send_sems.at[kv, f],
            recv_sem=recv_sems.at[0, kv, 0],
            device_id=partner,
            device_id_type=MESH,
        ).wait_send()

    def issue(c, f):
        for kv in range(2):
            flow_copy(c, kv, f).start()

    local = [
        pltpu.make_async_copy(q_hbm, q_v, q_sem),
        pltpu.make_async_copy(links_hbm, links, list_sems.at[0]),
        pltpu.make_async_copy(counts_hbm, counts, list_sems.at[1]),
    ]
    for copy in local:
        copy.start()
    pl.semaphore_wait(barrier, greeted)

    for f, (device, _, back) in enumerate(flows):

        @pl.when(before[f])
        def _():
            pl.semaphore_signal(
                ready.at[back], inc=1, device_id=device, device_id_type=MESH
            )
            issue(0, f)

    issue(0, beside)
    for f in (0, *range(2, beside), 1):

        @pl.when(jnp.logical_not(before[f]))
        def _():
            pl.semaphore_wait(ready.at[f], 1)
            issue(0, f)

    for c in range(1, chunks):
        for f in range(beside + 1):
            issue(c, f)
    for c in range(chunks):
        for kv in range(2):
            own_copy(c, kv).start()

    for copy in local:
        copy.wait()
    cand = lax.broadcasted_iota(jnp.int32, (1, slots * rows), 1) // tile_rows
    for i in range(tiles):
        used = jnp.where(cand == i, 1, 0)
        for j in range(lmax):
            hit = jnp.where(j < counts[i], links[i, j], -1)
            used = used + jnp.where(cand == hit, 1, 0)
        bias[i, :, :] = jnp.where(used == 0, -jnp.inf, jnp.where(used == 2, 1.0, 0.0))

    scale = HD ** (-0.5) * math.log2(math.e)

    def weigh(head):
        keys = land[0, :, :, head].reshape(slots * rows, HD)
        scores = lax.dot_general(
            q_v[:, head], keys, (((1,), (1,)), ((), ())), preferred_element_type=jnp.float32
        )
        scores = scores.reshape(tiles, tile_rows, slots * rows) * scale + bias[...]
        scores = scores.reshape(rows, slots * rows)
        weights = jnp.exp2(scores - jnp.max(scores, axis=1, keepdims=True))
        return weights.astype(jnp.bfloat16), jnp.sum(weights, axis=1, keepdims=True)

    def mix(head, weights, total):
        values = land[1, :, :, head].reshape(slots * rows, HD)
        mixed = jnp.dot(weights, values, preferred_element_type=jnp.float32)
        o_ref[:, head] = (mixed / total).astype(jnp.bfloat16)

    def attend(c):
        @pl.loop(bounds[c], bounds[c + 1])
        def _(h):
            head = pl.ds(pl.multiple_of(h * HD, HD), HD)
            mix(head, *weigh(head))

    def pass_beside(c, kv):
        arrived(c, kv, 4 - 3 * core)
        relay_copy(c, kv).start()

    def pass_across(c, kv):
        if crossed:
            arrived(c, kv, peer_slot(hops[kv][0], g))
            cross_copy(c, kv).start()

    def gather(c, kv):
        own_copy(c, kv).wait()
        if crossed:
            arrived(c, kv, peer_slot(hops[kv][1], g))
            arrived(c, kv, peer_slot(3 - g, g))
        else:
            for slot in range(5, slots):
                arrived(c, kv, slot)
        arrived(c, kv, 1 + 3 * core)
        for slot in (2, 3):
            arrived(c, kv, slot)

    last = chunks - 1
    for kv in range(2):
        pass_across(0, kv)
    for c in range(last):
        for kv in range(2):
            pass_beside(c, kv)
        for kv in range(2):
            pass_across(c + 1, kv)
        if c >= 1:
            for kv in range(2):
                gather(c - 1, kv)
            attend(c - 1)
    for kv in range(2):
        gather(last - 1, kv)
    attend(last - 1)

    heads = [pl.ds(h * HD, HD) for h in range(bounds[last], bounds[chunks])]
    pass_beside(last, 0)
    gather(last, 0)
    parts = [weigh(head) for head in heads]
    pass_beside(last, 1)
    gather(last, 1)
    for head, part in zip(heads, parts):
        mix(head, *part)

    for kv in range(2):
        for f in range(relay + 1 + crossed):
            sent(kv, f)


def shards(groups, ranks, *operands):
    queries, _, _, tile_links, link_counts = operands
    rows, features = queries.shape
    tiles = tile_links.shape[0]
    slots = 4 + groups
    heads = features // HD
    bounds = [0]
    for part in CHUNK_SIXTEENTHS:
        bounds.append(bounds[-1] + part * heads // 16)
    chunks = len(bounds) - 1
    hbm = pl.BlockSpec(memory_space=pl.ANY)
    return pl.pallas_call(
        functools.partial(kernel, groups, ranks, tuple(bounds)),
        out_shape=jax.ShapeDtypeStruct((rows, features), jnp.bfloat16),
        in_specs=[hbm] * 5,
        out_specs=pl.BlockSpec(memory_space=pltpu.VMEM),
        scratch_shapes=[
            pltpu.VMEM((2, slots, rows, features), jnp.bfloat16),
            pltpu.VMEM((rows, features), jnp.bfloat16),
            pltpu.VMEM((tiles, 1, slots * rows), jnp.float32),
            pltpu.SemaphoreType.DMA((2, groups + 4)),
            pltpu.SemaphoreType.DMA((chunks, 2, slots + 1)),
            pltpu.SemaphoreType.DMA,
            pltpu.SMEM(tile_links.shape, jnp.int32),
            pltpu.SMEM(link_counts.shape, jnp.int32),
            pltpu.SemaphoreType.DMA((2,)),
            pltpu.SemaphoreType.REGULAR((groups + 1,)),
        ],
        compiler_params=pltpu.CompilerParams(
            collective_id=0, has_side_effects=True, vmem_limit_bytes=28 * 2**20
        ),
    )(*(pltpu.with_memory_space_constraint(a, pltpu.HBM) for a in operands))


def solution(mesh):
    nodes = P(("group", "rank"), None)
    return jax.shard_map(
        functools.partial(shards, mesh.shape["group"], mesh.shape["rank"]),
        mesh=mesh,
        in_specs=(nodes, nodes, nodes, nodes, P(("group", "rank"))),
        out_specs=nodes,
        check_vma=False,
    )
```

```python
import functools
import math

import jax
import jax.numpy as jnp
from jax import lax
from jax.experimental import pallas as pl
from jax.experimental.pallas import tpu as pltpu
from jax.sharding import PartitionSpec as P

HD = 128
CHUNK_SIXTEENTHS = (9, 5, 1, 1)
MESH = pl.DeviceIdType.MESH
NEAR, ACROSS_K, ACROSS_V, REST, NEAR_V, REST_V, LATE = range(7)


def kernel(
    groups,
    ranks,
    bounds,
    q_hbm,
    k_hbm,
    v_hbm,
    links_hbm,
    counts_hbm,
    o_ref,
    land,
    q_v,
    bias,
    send_sem,
    recv_sems,
    ready,
    links,
    counts,
    local_sems,
):
    _, slots, rows, _ = land.shape
    chunks = len(bounds) - 1
    last = chunks - 1
    beat = min(1, last)
    tiles, lmax = links.shape
    tile_rows = rows // tiles
    g = lax.axis_index("group")
    r = lax.axis_index("rank")
    core = lax.rem(r, 2)
    partner = (g, r + 1 - 2 * core)
    crossed = groups == 4
    across = (g + 1 - 2 * lax.rem(g, 2), lax.rem(g + 2, 4))
    source = (k_hbm, v_hbm)

    def peer_slot(source, at):
        return 4 + lax.rem(source - at + groups, groups)

    flows = [
        ((g, lax.rem(r + 2, ranks)), 1, 1),
        ((g, lax.rem(r + ranks - 2, ranks)), 4, 0),
    ]
    if crossed:
        for other in across:
            flows.append(((other, r), peer_slot(g, other), len(flows)))
    else:
        for step in range(1, groups):
            back = 1 + groups - step
            flows.append(((lax.rem(g + groups - step, groups), r), 4 + step, back))
    hops = (across, across[::-1])
    near = 4 - 3 * core

    here = g * ranks + r
    before = [target[0] * ranks + target[1] < here for target, _, _ in flows]
    upper = 2 * r >= ranks
    inner = jnp.logical_and(r >= 2, r + 2 < ranks)
    second = [
        jnp.logical_and(inner, core == 0),
        jnp.logical_and(inner, core == 1),
        *(jnp.bool_(False) for _ in flows[2:]),
    ]
    barrier = pltpu.get_barrier_semaphore()
    pl.semaphore_signal(barrier, inc=1, device_id=partner, device_id_type=MESH)
    greeted = 1
    for (device, _, _), earlier in zip(flows, before):
        greeted = greeted + jnp.where(earlier, 1, 0)

        @pl.when(jnp.logical_not(earlier))
        def _():
            pl.semaphore_signal(barrier, inc=1, device_id=device, device_id_type=MESH)

    def columns(c):
        return pl.ds(bounds[c] * HD, (bounds[c + 1] - bounds[c]) * HD)

    def remote(src, dst, sem, device):
        return pltpu.make_async_remote_copy(
            src_ref=src,
            dst_ref=dst,
            send_sem=send_sem,
            recv_sem=sem,
            device_id=device,
            device_id_type=MESH,
        )

    def take(c, kind, ref):
        remote(ref, ref, recv_sems.at[c, kind], partner).wait_recv()

    def rest_of(c, kv):
        return REST_V if c == last and kv == 1 else REST

    def near_of(c, kv):
        return NEAR_V if c == last and kv == 1 else NEAR

    def flow(c, f):
        device, slot, _ = flows[f]
        for kv in range(2):
            if f < 2:
                other = LATE if c == last and kv == 1 else REST
                kind = jnp.where(core == 1 - f, near_of(c, kv), other)
            elif crossed and f - 2 == kv:
                kind = (ACROSS_K, ACROSS_V)[kv]
            else:
                kind = rest_of(c, kv)
            src = source[kv].at[:, columns(c)]
            dst = land.at[kv, slot, :, columns(c)]
            remote(src, dst, recv_sems.at[c, kind], device).start()

    def flow_beside(c):
        for kv in range(2):
            kind = NEAR_V if c == beat and c < last else rest_of(c, kv)
            src = source[kv].at[:, columns(c)]
            dst = land.at[kv, 2 + core, :, columns(c)]
            remote(src, dst, recv_sems.at[c, kind], partner).start()

    def pass_beside(c, kv=slice(None)):
        own = land.at[kv, near, :, columns(c)]
        take(c, NEAR if kv == slice(None) else near_of(c, kv), own)
        kind = REST if kv != 1 else LATE
        dst = land.at[kv, 3 - core, :, columns(c)]
        remote(own, dst, recv_sems.at[c, kind], partner).start()

    def pass_across(c):
        for kv in range(2 if crossed else 0):
            origin, target = hops[kv]
            own = land.at[kv, peer_slot(origin, g), :, columns(c)]
            take(c, (ACROSS_K, ACROSS_V)[kv], own)
            dst = land.at[kv, peer_slot(origin, target), :, columns(c)]
            remote(own, dst, recv_sems.at[c, rest_of(c, kv)], (target, r)).start()

    others = slots - 3 if crossed else slots - 2

    def gather(c):
        expected = others - 1 if c == beat and c < last else others
        take(c, REST, land.at[:, 0:expected, :, columns(c)])

    local = [
        pltpu.make_async_copy(src, dst, local_sems.at[i])
        for i, (src, dst) in enumerate(
            (
                (q_hbm, q_v),
                (links_hbm, links),
                (counts_hbm, counts),
                (k_hbm, land.at[0, 0]),
                (v_hbm, land.at[1, 0]),
            )
        )
    ]
    for copy in local[:3]:
        copy.start()
    pl.semaphore_wait(barrier, greeted)

    flow_beside(beat)
    for f, (device, _, back) in enumerate(flows):

        @pl.when(before[f])
        def _():
            pl.semaphore_signal(
                ready.at[back], inc=1, device_id=device, device_id_type=MESH
            )

        @pl.when(jnp.logical_and(before[f], jnp.logical_not(second[f])))
        def _():
            flow(0, f)

    for f in (0, *range(2, len(flows))):

        @pl.when(jnp.logical_not(before[f]))
        def _():
            pl.semaphore_wait(ready.at[f], 1)

        @pl.when(jnp.logical_not(jnp.logical_or(before[f], second[f])))
        def _():
            flow(0, f)

    if beat < last:
        take(beat, NEAR_V, land.at[:, 3 - core, :, columns(beat)])

    @pl.when(second[0])
    def _():
        flow(0, 0)

    @pl.when(jnp.logical_not(before[1]))
    def _():
        pl.semaphore_wait(ready.at[1], 1)

    @pl.when(jnp.logical_or(second[1], jnp.logical_not(before[1])))
    def _():
        flow(0, 1)

    for c in range(1, chunks):
        if c < last:
            flow(c, 0)
            flow(c, 1)
        else:

            @pl.when(upper)
            def _():
                flow(c, 0)
                flow(c, 1)

            @pl.when(jnp.logical_not(upper))
            def _():
                flow(c, 1)
                flow(c, 0)

        for f in range(2, len(flows)):
            flow(c, f)
    for c in range(chunks):
        if c != beat:
            flow_beside(c)
    for copy in local[3:]:
        copy.start()
    for copy in local:
        copy.wait()

    cand = lax.broadcasted_iota(jnp.int32, (1, slots * rows), 1) // tile_rows
    for i in range(tiles):
        used = jnp.where(cand == i, 1, 0)
        for j in range(lmax):
            hit = jnp.where(j < counts[i], links[i, j], -1)
            used = used + jnp.where(cand == hit, 1, 0)
        bias[i, :, :] = jnp.where(used == 0, -jnp.inf, jnp.where(used == 2, 1.0, 0.0))

    scale = HD ** (-0.5) * math.log2(math.e)

    def weigh(head):
        keys = land[0, :, :, head].reshape(slots * rows, HD)
        scores = lax.dot_general(
            q_v[:, head], keys, (((1,), (1,)), ((), ())), preferred_element_type=jnp.float32
        )
        scores = scores.reshape(tiles, tile_rows, slots * rows) * scale + bias[...]
        scores = scores.reshape(rows, slots * rows)
        weights = jnp.exp2(scores - jnp.max(scores, axis=1, keepdims=True))
        return weights.astype(jnp.bfloat16), jnp.sum(weights, axis=1, keepdims=True)

    def mix(head, weights, first, end):
        values = land[1, first:end, :, head].reshape((end - first) * rows, HD)
        part = weights[:, first * rows : end * rows]
        return jnp.dot(part, values, preferred_element_type=jnp.float32)

    def attend(heads):
        heads = [pl.ds(pl.multiple_of(h * HD, HD), HD) for h in heads]
        for head, (weights, total) in zip(heads, [weigh(head) for head in heads]):
            mixed = mix(head, weights, 0, slots)
            o_ref[:, head] = (mixed / total).astype(jnp.bfloat16)

    def attend_all(first, end):
        pairs = (end - first) // 2

        @pl.loop(0, pairs)
        def _(i):
            attend([first + 2 * i, first + 2 * i + 1])

        if first + 2 * pairs < end:
            attend([end - 1])

    pass_across(0)
    for c in range(last):
        pass_beside(c)
        pass_across(c + 1)
        gather(c)
        if c < last - 1:
            attend_all(bounds[c], bounds[c + 1])

    heads = [pl.ds(h * HD, HD) for h in range(bounds[last], bounds[chunks])]
    part = columns(last)
    middle = (bounds[last - 1] + bounds[last] + 1) // 2
    attend_all(bounds[last - 1], middle)
    pass_beside(last, 0)
    attend_all(middle, bounds[last])
    pass_beside(last, 1)
    take(last, REST, land.at[0, 0:others, :, part])
    weighed = [weigh(head) for head in heads]
    take(last, REST_V, land.at[1, 0 : others - 2, :, part])
    mixed = [
        mix(head, weights, 0, 1) + mix(head, weights, 5, slots)
        for head, (weights, _) in zip(heads, weighed)
    ]
    take(last, LATE, land.at[1, 0:2, :, part])
    for head, (weights, total), early in zip(heads, weighed, mixed):
        o_ref[:, head] = ((early + mix(head, weights, 1, 5)) / total).astype(jnp.bfloat16)

    everything = land.at[:, 0 : len(flows) + (3 if crossed else 2)]
    remote(everything, everything, recv_sems.at[0, 0], partner).wait_send()


def shards(groups, ranks, *operands):
    queries, _, _, tile_links, link_counts = operands
    rows, features = queries.shape
    tiles = tile_links.shape[0]
    slots = 4 + groups
    heads = features // HD
    bounds = [0]
    for part in CHUNK_SIXTEENTHS:
        bounds.append(bounds[-1] + part * heads // 16)
    chunks = len(bounds) - 1
    hbm = pl.BlockSpec(memory_space=pl.ANY)
    return pl.pallas_call(
        functools.partial(kernel, groups, ranks, tuple(bounds)),
        out_shape=jax.ShapeDtypeStruct((rows, features), jnp.bfloat16),
        in_specs=[hbm] * 5,
        out_specs=pl.BlockSpec(memory_space=pltpu.VMEM),
        scratch_shapes=[
            pltpu.VMEM((2, slots, rows, features), jnp.bfloat16),
            pltpu.VMEM((rows, features), jnp.bfloat16),
            pltpu.VMEM((tiles, 1, slots * rows), jnp.float32),
            pltpu.SemaphoreType.DMA,
            pltpu.SemaphoreType.DMA((chunks, 7)),
            pltpu.SemaphoreType.REGULAR((groups + 1,)),
            pltpu.SMEM(tile_links.shape, jnp.int32),
            pltpu.SMEM(link_counts.shape, jnp.int32),
            pltpu.SemaphoreType.DMA((5,)),
        ],
        compiler_params=pltpu.CompilerParams(
            collective_id=0, has_side_effects=True, vmem_limit_bytes=28 * 2**20
        ),
    )(*(pltpu.with_memory_space_constraint(a, pltpu.HBM) for a in operands))


def solution(mesh):
    nodes = P(("group", "rank"), None)
    return jax.shard_map(
        functools.partial(shards, mesh.shape["group"], mesh.shape["rank"]),
        mesh=mesh,
        in_specs=(nodes, nodes, nodes, nodes, P(("group", "rank"))),
        out_specs=nodes,
        check_vma=False,
    )
```

```python
import functools
import math

import jax
import jax.numpy as jnp
from jax import lax
from jax.experimental import pallas as pl
from jax.experimental.pallas import tpu as pltpu
from jax.sharding import PartitionSpec as P

HD = 128
CHUNK_SIXTEENTHS = (9, 5, 1, 1)
MESH = pl.DeviceIdType.MESH
NEAR, ACROSS_K, ACROSS_V, REST = range(4)
NEAR_V, REST_V, LATE, BEAT = range(4, 8)


def kernel(
    groups,
    ranks,
    bounds,
    q_hbm,
    k_hbm,
    v_hbm,
    links_hbm,
    counts_hbm,
    o_ref,
    land,
    q_v,
    bias,
    send_sem,
    recv_sems,
    ready,
    links,
    counts,
    local_sems,
):
    _, slots, rows, _ = land.shape
    chunks = len(bounds) - 1
    last = chunks - 1
    beat = min(1, last)
    tiles, lmax = links.shape
    tile_rows = rows // tiles
    g = lax.axis_index("group")
    r = lax.axis_index("rank")
    core = lax.rem(r, 2)
    partner = (g, r + 1 - 2 * core)
    crossed = groups == 4
    across = (g + 1 - 2 * lax.rem(g, 2), lax.rem(g + 2, 4))
    source = (k_hbm, v_hbm)

    def peer_slot(source, at):
        return 4 + lax.rem(source - at + groups, groups)

    flows = [
        ((g, lax.rem(r + 2, ranks)), 1, 1),
        ((g, lax.rem(r + ranks - 2, ranks)), 4, 0),
    ]
    if crossed:
        for other in across:
            flows.append(((other, r), peer_slot(g, other), len(flows)))
    else:
        for step in range(1, groups):
            back = 1 + groups - step
            flows.append(((lax.rem(g + groups - step, groups), r), 4 + step, back))
    hops = (across, across[::-1])
    near = 4 - 3 * core

    here = g * ranks + r
    before = [target[0] * ranks + target[1] < here for target, _, _ in flows]
    upper = 2 * r >= ranks
    inner = jnp.logical_and(r >= 2, r + 2 < ranks)
    second = [
        jnp.logical_and(inner, core == 0),
        jnp.logical_and(inner, core == 1),
        *(jnp.bool_(False) for _ in flows[2:]),
    ]
    barrier = pltpu.get_barrier_semaphore()
    pl.semaphore_signal(barrier, inc=1, device_id=partner, device_id_type=MESH)
    greeted = 1
    for (device, _, _), earlier in zip(flows, before):
        greeted = greeted + jnp.where(earlier, 1, 0)

        @pl.when(jnp.logical_not(earlier))
        def _():
            pl.semaphore_signal(barrier, inc=1, device_id=device, device_id_type=MESH)

    def columns(c):
        return pl.ds(bounds[c] * HD, (bounds[c + 1] - bounds[c]) * HD)

    def remote(src, dst, sem, device):
        return pltpu.make_async_remote_copy(
            src_ref=src,
            dst_ref=dst,
            send_sem=send_sem,
            recv_sem=sem,
            device_id=device,
            device_id_type=MESH,
        )

    def mark(c, kind):
        return recv_sems.at[kind + 4 * c]

    def take(c, kind, ref):
        remote(ref, ref, mark(c, kind), partner).wait_recv()

    def rest_of(c, kv):
        return REST_V if c == last and kv == 1 else REST

    def near_of(c, kv):
        return NEAR_V if c == last and kv == 1 else NEAR

    def flow(c, f):
        device, slot, _ = flows[f]
        for kv in range(2):
            if f < 2:
                other = LATE if c == last and kv == 1 else REST
                kind = jnp.where(core == 1 - f, near_of(c, kv), other)
            elif crossed and f - 2 == kv:
                kind = (ACROSS_K, ACROSS_V)[kv]
            else:
                kind = rest_of(c, kv)
            src = source[kv].at[:, columns(c)]
            dst = land.at[kv, slot, :, columns(c)]
            remote(src, dst, mark(c, kind), device).start()

    def flow_beside(c):
        for kv in range(2):
            kind = BEAT if c == beat and c < last else rest_of(c, kv)
            src = source[kv].at[:, columns(c)]
            dst = land.at[kv, 2 + core, :, columns(c)]
            remote(src, dst, mark(last if kind == BEAT else c, kind), partner).start()

    def pass_beside(c, kv=slice(None)):
        own = land.at[kv, near, :, columns(c)]
        take(c, NEAR if kv == slice(None) else near_of(c, kv), own)
        kind = REST if kv != 1 else LATE
        dst = land.at[kv, 3 - core, :, columns(c)]
        remote(own, dst, mark(c, kind), partner).start()

    def pass_across(c):
        for kv in range(2 if crossed else 0):
            origin, target = hops[kv]
            own = land.at[kv, peer_slot(origin, g), :, columns(c)]
            take(c, (ACROSS_K, ACROSS_V)[kv], own)
            dst = land.at[kv, peer_slot(origin, target), :, columns(c)]
            remote(own, dst, mark(c, rest_of(c, kv)), (target, r)).start()

    others = slots - 3 if crossed else slots - 2

    def gather(c):
        expected = others - 1 if c == beat and c < last else others
        take(c, REST, land.at[:, 0:expected, :, columns(c)])

    local = [
        pltpu.make_async_copy(src, dst, local_sems.at[i])
        for i, (src, dst) in enumerate(
            (
                (q_hbm, q_v),
                (links_hbm, links),
                (counts_hbm, counts),
                (k_hbm, land.at[0, 0]),
                (v_hbm, land.at[1, 0]),
            )
        )
    ]
    for copy in local[:3]:
        copy.start()
    pl.semaphore_wait(barrier, greeted)

    flow_beside(beat)
    for f, (device, _, back) in enumerate(flows):

        @pl.when(before[f])
        def _():
            pl.semaphore_signal(
                ready.at[back], inc=1, device_id=device, device_id_type=MESH
            )

        @pl.when(jnp.logical_and(before[f], jnp.logical_not(second[f])))
        def _():
            flow(0, f)

    for f in (0, *range(2, len(flows))):

        @pl.when(jnp.logical_not(before[f]))
        def _():
            pl.semaphore_wait(ready.at[f], 1)

        @pl.when(jnp.logical_not(jnp.logical_or(before[f], second[f])))
        def _():
            flow(0, f)

    if beat < last:
        take(last, BEAT, land.at[:, 3 - core, :, columns(beat)])

    @pl.when(second[0])
    def _():
        flow(0, 0)

    @pl.when(jnp.logical_not(before[1]))
    def _():
        pl.semaphore_wait(ready.at[1], 1)

    @pl.when(jnp.logical_or(second[1], jnp.logical_not(before[1])))
    def _():
        flow(0, 1)

    for c in range(1, chunks):
        if c < last:
            flow(c, 0)
            flow(c, 1)
        else:

            @pl.when(upper)
            def _():
                flow(c, 0)
                flow(c, 1)

            @pl.when(jnp.logical_not(upper))
            def _():
                flow(c, 1)
                flow(c, 0)

        for f in range(2, len(flows)):
            flow(c, f)
    for c in range(chunks):
        if c != beat:
            flow_beside(c)
    for copy in local[3:]:
        copy.start()
    for copy in local:
        copy.wait()

    cand = lax.broadcasted_iota(jnp.int32, (1, slots * rows), 1) // tile_rows
    for i in range(tiles):
        used = jnp.where(cand == i, 1, 0)
        for j in range(lmax):
            hit = jnp.where(j < counts[i], links[i, j], -1)
            used = used + jnp.where(cand == hit, 1, 0)
        bias[i, :, :] = jnp.where(used == 0, -jnp.inf, jnp.where(used == 2, 1.0, 0.0))

    scale = HD ** (-0.5) * math.log2(math.e)

    def weigh(head):
        keys = land[0, :, :, head].reshape(slots * rows, HD)
        scores = lax.dot_general(
            q_v[:, head], keys, (((1,), (1,)), ((), ())), preferred_element_type=jnp.float32
        )
        scores = scores.reshape(tiles, tile_rows, slots * rows) * scale + bias[...]
        scores = scores.reshape(rows, slots * rows)
        weights = jnp.exp2(scores - jnp.max(scores, axis=1, keepdims=True))
        return weights.astype(jnp.bfloat16), jnp.sum(weights, axis=1, keepdims=True)

    def mix(head, weights, first, end):
        values = land[1, first:end, :, head].reshape((end - first) * rows, HD)
        part = weights[:, first * rows : end * rows]
        return jnp.dot(part, values, preferred_element_type=jnp.float32)

    def attend(heads):
        heads = [pl.ds(pl.multiple_of(h * HD, HD), HD) for h in heads]
        for head, (weights, total) in zip(heads, [weigh(head) for head in heads]):
            mixed = mix(head, weights, 0, slots)
            o_ref[:, head] = (mixed / total).astype(jnp.bfloat16)

    def attend_all(first, end):
        pairs = (end - first) // 2
        if pairs > 0:

            @pl.loop(0, pairs)
            def _(i):
                attend([first + 2 * i, first + 2 * i + 1])

        if first + 2 * pairs < end:
            attend([end - 1])

    pass_across(0)
    for c in range(last):
        pass_beside(c)
        pass_across(c + 1)
        gather(c)
        if c < last - 1:
            attend_all(bounds[c], bounds[c + 1])

    heads = [pl.ds(h * HD, HD) for h in range(bounds[last], bounds[chunks])]
    part = columns(last)
    middle = (bounds[last - 1] + bounds[last]) // 2
    attend_all(bounds[last - 1], middle)
    pass_beside(last, 0)
    attend_all(middle, bounds[last])
    pass_beside(last, 1)
    take(last, REST, land.at[0, 0:others, :, part])
    weighed = [weigh(head) for head in heads]
    take(last, REST_V, land.at[1, 0 : others - 2, :, part])
    mixed = [
        mix(head, weights, 0, 1) + mix(head, weights, 5, slots)
        for head, (weights, _) in zip(heads, weighed)
    ]
    take(last, LATE, land.at[1, 0:2, :, part])
    for head, (weights, total), early in zip(heads, weighed, mixed):
        o_ref[:, head] = ((early + mix(head, weights, 1, 5)) / total).astype(jnp.bfloat16)

    everything = land.at[:, 0 : len(flows) + (3 if crossed else 2)]
    remote(everything, everything, recv_sems.at[0], partner).wait_send()


def shards(groups, ranks, *operands):
    queries, _, _, tile_links, link_counts = operands
    rows, features = queries.shape
    tiles = tile_links.shape[0]
    slots = 4 + groups
    heads = features // HD
    bounds = [0]
    for part in CHUNK_SIXTEENTHS:
        bounds.append(bounds[-1] + part * heads // 16)
    chunks = len(bounds) - 1
    hbm = pl.BlockSpec(memory_space=pl.ANY)
    return pl.pallas_call(
        functools.partial(kernel, groups, ranks, tuple(bounds)),
        out_shape=jax.ShapeDtypeStruct((rows, features), jnp.bfloat16),
        in_specs=[hbm] * 5,
        out_specs=pl.BlockSpec(memory_space=pltpu.VMEM),
        scratch_shapes=[
            pltpu.VMEM((2, slots, rows, features), jnp.bfloat16),
            pltpu.VMEM((rows, features), jnp.bfloat16),
            pltpu.VMEM((tiles, 1, slots * rows), jnp.float32),
            pltpu.SemaphoreType.DMA,
            pltpu.SemaphoreType.DMA((4 * chunks + 4,)),
            pltpu.SemaphoreType.REGULAR((groups + 1,)),
            pltpu.SMEM(tile_links.shape, jnp.int32),
            pltpu.SMEM(link_counts.shape, jnp.int32),
            pltpu.SemaphoreType.DMA((5,)),
        ],
        compiler_params=pltpu.CompilerParams(
            collective_id=0, has_side_effects=True, vmem_limit_bytes=28 * 2**20
        ),
    )(*(pltpu.with_memory_space_constraint(a, pltpu.HBM) for a in operands))


def solution(mesh):
    nodes = P(("group", "rank"), None)
    return jax.shard_map(
        functools.partial(shards, mesh.shape["group"], mesh.shape["rank"]),
        mesh=mesh,
        in_specs=(nodes, nodes, nodes, nodes, P(("group", "rank"))),
        out_specs=nodes,
        check_vma=False,
    )
```

```python
import functools
import math

import jax
import jax.numpy as jnp
from jax import lax
from jax.experimental import pallas as pl
from jax.experimental.pallas import tpu as pltpu
from jax.sharding import PartitionSpec as P

HD = 128
CHUNK_SIXTEENTHS = (9, 5, 1, 1)
MESH = pl.DeviceIdType.MESH
NEAR, ACROSS_K, ACROSS_V, REST = range(4)
NEAR_V, REST_V, LATE, BEAT = range(4, 8)


def kernel(
    groups,
    ranks,
    bounds,
    q_hbm,
    k_hbm,
    v_hbm,
    links_hbm,
    counts_hbm,
    o_ref,
    land,
    q_v,
    bias,
    send_sem,
    recv_sems,
    ready,
    links,
    counts,
    local_sems,
):
    _, slots, rows, _ = land.shape
    chunks = len(bounds) - 1
    last = chunks - 1
    beat = min(1, last)
    tiles, lmax = links.shape
    tile_rows = rows // tiles
    g = lax.axis_index("group")
    r = lax.axis_index("rank")
    core = lax.rem(r, 2)
    partner = (g, r + 1 - 2 * core)
    crossed = groups == 4
    across = (g + 1 - 2 * lax.rem(g, 2), lax.rem(g + 2, 4))
    source = (k_hbm, v_hbm)

    def peer_slot(source, at):
        return 4 + lax.rem(source - at + groups, groups)

    flows = [
        ((g, lax.rem(r + 2, ranks)), 1, 1),
        ((g, lax.rem(r + ranks - 2, ranks)), 4, 0),
    ]
    if crossed:
        for other in across:
            flows.append(((other, r), peer_slot(g, other), len(flows)))
    else:
        for step in range(1, groups):
            back = 1 + groups - step
            flows.append(((lax.rem(g + groups - step, groups), r), 4 + step, back))
    hops = (across, across[::-1])
    near = 4 - 3 * core

    here = g * ranks + r
    before = [target[0] * ranks + target[1] < here for target, _, _ in flows]
    upper = 2 * r >= ranks
    inner = jnp.logical_and(r >= 2, r + 2 < ranks)
    second = [
        jnp.logical_and(inner, core == 0),
        jnp.logical_and(inner, core == 1),
        *(jnp.bool_(False) for _ in flows[2:]),
    ]
    barrier = pltpu.get_barrier_semaphore()
    pl.semaphore_signal(barrier, inc=1, device_id=partner, device_id_type=MESH)
    greeted = 1
    for (device, _, _), earlier in zip(flows, before):
        greeted = greeted + jnp.where(earlier, 1, 0)

        @pl.when(jnp.logical_not(earlier))
        def _():
            pl.semaphore_signal(barrier, inc=1, device_id=device, device_id_type=MESH)

    def columns(c):
        return pl.ds(bounds[c] * HD, (bounds[c + 1] - bounds[c]) * HD)

    def remote(src, dst, sem, device):
        return pltpu.make_async_remote_copy(
            src_ref=src,
            dst_ref=dst,
            send_sem=send_sem,
            recv_sem=sem,
            device_id=device,
            device_id_type=MESH,
        )

    def mark(c, kind):
        return recv_sems.at[kind + 4 * c]

    def take(c, kind, ref):
        remote(ref, ref, mark(c, kind), partner).wait_recv()

    def rest_of(c, kv):
        return REST_V if c == last and kv == 1 else REST

    def near_of(c, kv):
        return NEAR_V if c == last and kv == 1 else NEAR

    def flow(c, f):
        device, slot, _ = flows[f]
        for kv in range(2):
            if f < 2:
                other = LATE if c == last and kv == 1 else REST
                kind = jnp.where(core == 1 - f, near_of(c, kv), other)
            elif crossed and f - 2 == kv:
                kind = (ACROSS_K, ACROSS_V)[kv]
            else:
                kind = rest_of(c, kv)
            src = source[kv].at[:, columns(c)]
            dst = land.at[kv, slot, :, columns(c)]
            remote(src, dst, mark(c, kind), device).start()

    def flow_beside(c):
        for kv in range(2):
            kind = BEAT if c == beat and c < last else rest_of(c, kv)
            src = source[kv].at[:, columns(c)]
            dst = land.at[kv, 2 + core, :, columns(c)]
            remote(src, dst, mark(last if kind == BEAT else c, kind), partner).start()

    def pass_beside(c, kv=slice(None)):
        own = land.at[kv, near, :, columns(c)]
        take(c, NEAR if kv == slice(None) else near_of(c, kv), own)
        kind = REST if kv != 1 else LATE
        dst = land.at[kv, 3 - core, :, columns(c)]
        remote(own, dst, mark(c, kind), partner).start()

    def pass_across(c):
        for kv in range(2 if crossed else 0):
            origin, target = hops[kv]
            own = land.at[kv, peer_slot(origin, g), :, columns(c)]
            take(c, (ACROSS_K, ACROSS_V)[kv], own)
            dst = land.at[kv, peer_slot(origin, target), :, columns(c)]
            remote(own, dst, mark(c, rest_of(c, kv)), (target, r)).start()

    others = slots - 3 if crossed else slots - 2

    def gather(c):
        expected = others - 1 if c == beat and c < last else others
        take(c, REST, land.at[:, 0:expected, :, columns(c)])

    local = [
        pltpu.make_async_copy(src, dst, local_sems.at[min(i, 3)])
        for i, (src, dst) in enumerate(
            (
                (q_hbm, q_v),
                (links_hbm, links),
                (counts_hbm, counts),
                (k_hbm, land.at[0, 0]),
                (v_hbm, land.at[1, 0]),
            )
        )
    ]
    for copy in local[:3]:
        copy.start()
    pl.semaphore_wait(barrier, greeted)

    flow_beside(beat)
    for f, (device, _, back) in enumerate(flows):

        @pl.when(before[f])
        def _():
            pl.semaphore_signal(
                ready.at[back], inc=1, device_id=device, device_id_type=MESH
            )

        @pl.when(jnp.logical_and(before[f], jnp.logical_not(second[f])))
        def _():
            flow(0, f)

    for f in (0, *range(2, len(flows))):

        @pl.when(jnp.logical_not(before[f]))
        def _():
            pl.semaphore_wait(ready.at[f], 1)

        @pl.when(jnp.logical_not(jnp.logical_or(before[f], second[f])))
        def _():
            flow(0, f)

    if beat < last:
        take(last, BEAT, land.at[:, 3 - core, :, columns(beat)])

    @pl.when(second[0])
    def _():
        flow(0, 0)

    @pl.when(jnp.logical_not(before[1]))
    def _():
        pl.semaphore_wait(ready.at[1], 1)

    @pl.when(jnp.logical_or(second[1], jnp.logical_not(before[1])))
    def _():
        flow(0, 1)

    for c in range(1, chunks):
        if c < last:
            flow(c, 0)
            flow(c, 1)
        else:

            @pl.when(upper)
            def _():
                flow(c, 0)
                flow(c, 1)

            @pl.when(jnp.logical_not(upper))
            def _():
                flow(c, 1)
                flow(c, 0)

        for f in range(2, len(flows)):
            flow(c, f)
    for c in range(chunks):
        if c != beat:
            flow_beside(c)
    for copy in local[3:]:
        copy.start()
    for copy in local[:3]:
        copy.wait()
    own = land.at[:, 0]
    pltpu.make_async_copy(own, own, local_sems.at[3]).wait()

    cand = lax.broadcasted_iota(jnp.int32, (1, slots * rows), 1) // tile_rows
    for i in range(tiles):
        used = jnp.where(cand == i, 1, 0)
        for j in range(lmax):
            hit = jnp.where(j < counts[i], links[i, j], -1)
            used = used + jnp.where(cand == hit, 1, 0)
        bias[i, :, :] = jnp.where(used == 0, -jnp.inf, jnp.where(used == 2, 1.0, 0.0))

    scale = HD ** (-0.5) * math.log2(math.e)

    def weigh(head):
        keys = land[0, :, :, head].reshape(slots * rows, HD)
        scores = lax.dot_general(
            q_v[:, head], keys, (((1,), (1,)), ((), ())), preferred_element_type=jnp.float32
        )
        scores = scores.reshape(tiles, tile_rows, slots * rows) * scale + bias[...]
        scores = scores.reshape(rows, slots * rows)
        weights = jnp.exp2(scores - jnp.max(scores, axis=1, keepdims=True))
        return weights.astype(jnp.bfloat16), jnp.sum(weights, axis=1, keepdims=True)

    def mix(head, weights, first, end):
        values = land[1, first:end, :, head].reshape((end - first) * rows, HD)
        part = weights[:, first * rows : end * rows]
        return jnp.dot(part, values, preferred_element_type=jnp.float32)

    def attend(heads):
        heads = [pl.ds(pl.multiple_of(h * HD, HD), HD) for h in heads]
        for head, (weights, total) in zip(heads, [weigh(head) for head in heads]):
            mixed = mix(head, weights, 0, slots)
            o_ref[:, head] = (mixed / total).astype(jnp.bfloat16)

    def attend_all(first, end):
        pairs = (end - first) // 2
        if pairs > 0:

            @pl.loop(0, pairs)
            def _(i):
                attend([first + 2 * i, first + 2 * i + 1])

        if first + 2 * pairs < end:
            attend([end - 1])

    pass_across(0)
    for c in range(last):
        pass_beside(c)
        pass_across(c + 1)
        gather(c)
        if c < last - 1:
            attend_all(bounds[c], bounds[c + 1])

    heads = [pl.ds(h * HD, HD) for h in range(bounds[last], bounds[chunks])]
    part = columns(last)
    middle = (bounds[last - 1] + bounds[last]) // 2
    attend_all(bounds[last - 1], middle)
    pass_beside(last, 0)
    attend_all(middle, bounds[last])
    pass_beside(last, 1)
    take(last, REST, land.at[0, 0:others, :, part])
    weighed = [weigh(head) for head in heads]
    take(last, REST_V, land.at[1, 0 : others - 2, :, part])
    mixed = [
        mix(head, weights, 0, 1) + mix(head, weights, 5, slots)
        for head, (weights, _) in zip(heads, weighed)
    ]
    take(last, LATE, land.at[1, 0:2, :, part])
    for head, (weights, total), early in zip(heads, weighed, mixed):
        o_ref[:, head] = ((early + mix(head, weights, 1, 5)) / total).astype(jnp.bfloat16)

    everything = land.at[:, 0 : len(flows) + (3 if crossed else 2)]
    remote(everything, everything, recv_sems.at[0], partner).wait_send()


def shards(groups, ranks, *operands):
    queries, _, _, tile_links, link_counts = operands
    rows, features = queries.shape
    tiles = tile_links.shape[0]
    slots = 4 + groups
    heads = features // HD
    bounds = [0]
    for part in CHUNK_SIXTEENTHS:
        bounds.append(bounds[-1] + part * heads // 16)
    chunks = len(bounds) - 1
    hbm = pl.BlockSpec(memory_space=pl.ANY)
    attended = pl.pallas_call(
        functools.partial(kernel, groups, ranks, tuple(bounds)),
        out_shape=jax.ShapeDtypeStruct((rows, features), jnp.bfloat16),
        in_specs=[hbm] * 5,
        out_specs=pl.BlockSpec(memory_space=pltpu.VMEM),
        scratch_shapes=[
            pltpu.VMEM((2, slots, rows, features), jnp.bfloat16),
            pltpu.VMEM((rows, features), jnp.bfloat16),
            pltpu.VMEM((tiles, 1, slots * rows), jnp.float32),
            pltpu.SemaphoreType.DMA,
            pltpu.SemaphoreType.DMA((4 * chunks + 4,)),
            pltpu.SemaphoreType.REGULAR((4 if groups == 4 else groups + 1,)),
            pltpu.SMEM(tile_links.shape, jnp.int32),
            pltpu.SMEM(link_counts.shape, jnp.int32),
            pltpu.SemaphoreType.DMA((4,)),
        ],
        compiler_params=pltpu.CompilerParams(
            collective_id=0, has_side_effects=True, vmem_limit_bytes=28 * 2**20
        ),
    )(*(pltpu.with_memory_space_constraint(a, pltpu.HBM) for a in operands))

    def write(src, dst, sems):
        parts = src.shape[0] // sems.shape[0]
        copies = [
            pltpu.make_async_copy(
                src.at[pl.ds(i * parts, parts)], dst.at[pl.ds(i * parts, parts)], sems.at[i]
            )
            for i in range(sems.shape[0])
        ]
        for copy in copies:
            copy.start()
        for copy in copies:
            copy.wait()

    return pl.pallas_call(
        write,
        out_shape=jax.ShapeDtypeStruct(attended.shape, attended.dtype),
        in_specs=[pl.BlockSpec(memory_space=pltpu.VMEM)],
        out_specs=hbm,
        scratch_shapes=[pltpu.SemaphoreType.DMA((1,))],
        compiler_params=pltpu.CompilerParams(vmem_limit_bytes=2**20),
    )(attended)


def solution(mesh):
    nodes = P(("group", "rank"), None)
    return jax.shard_map(
        functools.partial(shards, mesh.shape["group"], mesh.shape["rank"]),
        mesh=mesh,
        in_specs=(nodes, nodes, nodes, nodes, P(("group", "rank"))),
        out_specs=nodes,
        check_vma=False,
    )
```
